32 devices in a mesh: depth: 2 (over x), row: 4 (over y, core), col: 4 (over z).
Axes of the slice: x: 2, y: 2, z: 4, core: 2. Of those that a mesh axis runs over, the one named last changes fastest.
Arguments:
- tokens: bfloat16 [128, 8192], P('row', ('depth', 'col')), may hold values from -6 to 6
- cotangent: bfloat16 [128, 8192], P('row', ('depth', 'col')), may hold values from -6 to 6
- gate_weight: bfloat16 [8192, 29568], P(('depth', 'col'), 'row'), may hold values from -0.0625 to 0.0625
- up_weight: bfloat16 [8192, 29568], P(('depth', 'col'), 'row'), may hold values from -0.0625 to 0.0625
- down_weight: bfloat16 [29568, 8192], P('row', ('depth', 'col')), may hold values from -0.03125 to 0.03125
Outputs:
- input_grad: bfloat16 [128, 8192], P('row', ('depth', 'col'))
- gate_weight_grad: bfloat16 [8192, 29568], P(('depth', 'col'), 'row')
- up_weight_grad: bfloat16 [8192, 29568], P(('depth', 'col'), 'row')
- down_weight_grad: bfloat16 [29568, 8192], P('row', ('depth', 'col'))
The draws below stay inside these ranges and needn't reach their ends.
All inputs are finite; a program needn't handle non-finite values.
Results may differ from the reference program's by a relative error of at most 0.00235.
Values may be sent and summed in bfloat16 or wider, within the bound.
A program may use at most 192 MiB of HBM per device.

```python
import jax
import jax.numpy as jnp

D = 8192
FF = 29568
TOKENS = 128


def block_levels(stream_key, extent, pieces, low, top_value):
    gain, own = 1.0, jax.random.fold_in(stream_key, 6)
    for axis_at, blocks in pieces:
        steps = jnp.exp(jax.random.uniform(jax.random.fold_in(own, axis_at), (blocks,), jnp.float32, low / len(pieces), top_value / len(pieces)))
        gain = gain * jnp.repeat(steps, extent[axis_at] // blocks).reshape([-1 if axis == axis_at else 1 for axis in range(len(extent))])
    return gain


def normal_values(stream_key, extent, spread, limit, pieces=(), kind=jnp.bfloat16):
    factor_of = block_levels(stream_key, extent, pieces, -0.22, 0.18) if pieces else 1.0
    values = jax.random.normal(stream_key, extent, jnp.float32) * spread * factor_of
    return jnp.minimum(jnp.maximum(values, -limit), limit).astype(kind)


def setup_inputs(seed: int = 0) -> dict:
    key_of = jax.random.split(jax.random.key(seed), 6)
    tokens = normal_values(key_of[0], (TOKENS, D), 1.0, 6.0, ((0, 4), (1, 8)))
    cotangent = normal_values(key_of[1], (TOKENS, D), 0.5, 6.0, ((0, 4), (1, 8)))
    gate_weight = normal_values(key_of[2], (D, FF), D ** -0.5, 0.0625, ((0, 8), (1, 4)))
    up_weight = normal_values(key_of[3], (D, FF), D ** -0.5, 0.0625, ((0, 8), (1, 4)))
    down_weight = normal_values(key_of[4], (FF, D), FF ** -0.5, 0.03125, ((0, 4), (1, 8)))
    return {"tokens": tokens, "cotangent": cotangent, "gate_weight": gate_weight, "up_weight": up_weight, "down_weight": down_weight}


def reference(tokens, cotangent, gate_weight, up_weight, down_weight):
    gate_sum = jnp.dot(tokens, gate_weight, preferred_element_type=jnp.float32)
    up_sum = jnp.dot(tokens, up_weight, preferred_element_type=jnp.float32)
    back_sum = jnp.dot(cotangent, down_weight.T, preferred_element_type=jnp.float32)
    sigmoid = jax.nn.sigmoid(gate_sum)
    hidden = (gate_sum * sigmoid * up_sum).astype(jnp.bfloat16)
    gate_grad = (back_sum * up_sum * sigmoid * (1.0 + gate_sum * (1.0 - sigmoid))).astype(jnp.bfloat16)
    up_grad = (back_sum * gate_sum * sigmoid).astype(jnp.bfloat16)
    down_weight_grad = jnp.dot(hidden.T, cotangent, preferred_element_type=jnp.float32).astype(jnp.bfloat16)
    gate_weight_grad = jnp.dot(tokens.T, gate_grad, preferred_element_type=jnp.float32).astype(jnp.bfloat16)
    up_weight_grad = jnp.dot(tokens.T, up_grad, preferred_element_type=jnp.float32).astype(jnp.bfloat16)
    input_sum = jnp.dot(gate_grad, gate_weight.T, preferred_element_type=jnp.float32)
    input_sum = input_sum + jnp.dot(up_grad, up_weight.T, preferred_element_type=jnp.float32)
    return input_sum.astype(jnp.bfloat16), gate_weight_grad, up_weight_grad, down_weight_grad
```

```python
import math

import jax
import jax.numpy as jnp
from jax import lax
from jax.sharding import PartitionSpec as P

CHUNKS = 4
TOKEN_MAX = 6.0
WEIGHT_MAX = 0.0625
HALF_MAX = 65504.0


def ring(n, shift):
    return [((i + shift) % n, i) for i in range(n)]


def from_peer(x, axis, n, shift):
    return lax.ppermute(x, axis, ring(n, shift))


def over_rows(left, right):
    return lax.dot_general(
        left, right, (((0,), (0,)), ((), ())), preferred_element_type=jnp.float32
    )


def over_columns(left, right):
    return lax.dot_general(
        left, right, (((1,), (1,)), ((), ())), preferred_element_type=jnp.float32
    )


def hidden_terms(gate_sum, up_sum, back_sum):
    sigmoid = jax.nn.sigmoid(gate_sum)
    hidden = (gate_sum * sigmoid * up_sum).astype(jnp.bfloat16)
    gate_grad = (back_sum * up_sum * sigmoid * (1.0 + gate_sum * (1.0 - sigmoid))).astype(
        jnp.bfloat16
    )
    up_grad = (back_sum * gate_sum * sigmoid).astype(jnp.bfloat16)
    return (gate_grad, up_grad, hidden)


def chunk_bounds(units):
    tiles = -(-units // 128)
    edges = [min(units, 128 * (tiles * i // CHUNKS)) for i in range(CHUNKS + 1)]
    edges[-1] = units
    return list(zip(edges[:-1], edges[1:]))


def build(depth_n, row_n, col_n):
    def shards(tokens, cotangent, gate_weight, up_weight, down_weight):
        width, units = gate_weight.shape
        local = tokens.shape[0]
        count = local * row_n
        block = count // (depth_n * col_n)
        half = block * col_n
        bound = depth_n * width * TOKEN_MAX * WEIGHT_MAX
        scale = 2.0 ** math.floor(math.log2(HALF_MAX / bound))
        my_depth, my_col = lax.axis_index("depth"), lax.axis_index("col")

        both = jnp.stack([tokens, cotangent])
        both = jnp.concatenate(
            [both] + [from_peer(both, "row", row_n, k) for k in range(1, row_n)], axis=1
        )
        both = both.reshape(2, depth_n, col_n, block, width)
        both = jnp.roll(jnp.roll(both, -my_depth, axis=1), -my_col, axis=2)
        both = both.reshape(2, count, width)
        tok, cot = both[0], both[1]

        pieces = []
        for low, high in chunk_bounds(units):
            parts = (
                jnp.dot(tok, gate_weight[:, low:high], preferred_element_type=jnp.float32),
                jnp.dot(tok, up_weight[:, low:high], preferred_element_type=jnp.float32),
                over_columns(cot, down_weight[low:high]),
            )
            part = jnp.stack([(p * scale).astype(jnp.float16) for p in parts])
            total = part[:, :half].astype(jnp.float32)
            for k in range(1, depth_n):
                away = part[:, k * half : (k + 1) * half]
                total = total + lax.ppermute(
                    away, "depth", [(i, (i + k) % depth_n) for i in range(depth_n)]
                ).astype(jnp.float32)
            layer = total.astype(jnp.float16)
            total = total[:, :block]
            for k in range(1, col_n):
                away = layer[:, k * block : (k + 1) * block]
                total = total + lax.ppermute(
                    away, "col", [(i, (i + k) % col_n) for i in range(col_n)]
                ).astype(jnp.float32)
            total = total * (1.0 / scale)
            piece = jnp.stack(hidden_terms(total[0], total[1], total[2]))
            wider = jnp.concatenate(
                [piece] + [from_peer(piece, "col", col_n, k) for k in range(1, col_n)], axis=1
            )
            whole = jnp.concatenate(
                [wider] + [from_peer(wider, "depth", depth_n, k) for k in range(1, depth_n)],
                axis=1,
            )
            pieces.append(whole)
        full = jnp.concatenate(pieces, axis=2)
        gate_grad, up_grad, hidden = full[0], full[1], full[2]
        rows = over_columns(gate_grad, gate_weight) + over_columns(up_grad, up_weight)
        rows = rows.reshape(depth_n, col_n, block, width)
        rows = jnp.roll(jnp.roll(rows, my_depth, axis=0), my_col, axis=1)
        rows = rows.reshape(row_n, local, width)
        input_sum = rows[0]
        for k in range(1, row_n):
            input_sum = input_sum + lax.ppermute(
                rows[k], "row", [(i, (i + k) % row_n) for i in range(row_n)]
            )
        return (
            input_sum.astype(jnp.bfloat16),
            over_rows(tok, gate_grad).astype(jnp.bfloat16),
            over_rows(tok, up_grad).astype(jnp.bfloat16),
            over_rows(hidden, cot).astype(jnp.bfloat16),
        )

    return shards


def solution(mesh):
    return jax.shard_map(
        build(mesh.shape["depth"], mesh.shape["row"], mesh.shape["col"]),
        mesh=mesh,
        in_specs=(
            P("row", ("depth", "col")),
            P("row", ("depth", "col")),
            P(("depth", "col"), "row"),
            P(("depth", "col"), "row"),
            P("row", ("depth", "col")),
        ),
        out_specs=(
            P("row", ("depth", "col")),
            P(("depth", "col"), "row"),
            P(("depth", "col"), "row"),
            P("row", ("depth", "col")),
        ),
        check_vma=False,
    )
```

```python
import math

import jax
import jax.numpy as jnp
from jax import lax
from jax.sharding import PartitionSpec as P


CHUNKS = 4
TOKEN_MAX = 6.0
WEIGHT_MAX = 0.0625
HALF_MAX = 65504.0


def ring(n, shift):
    return [((i + shift) % n, i) for i in range(n)]


def doubled(n):
    order, step = [0], n // 2
    while step:
        order = order + [m ^ step for m in order]
        step //= 2
    return order


def place(mask, n):
    out, bits = 0 * mask, n.bit_length() - 1
    for bit in range(bits):
        out = out + ((mask >> bit) & 1) * (1 << (bits - 1 - bit))
    return out


def swap(x, axis, n, mask):
    return lax.ppermute(x, axis, [(i, i ^ mask) for i in range(n)])


def from_peer(x, axis, n, shift):
    return lax.ppermute(x, axis, ring(n, shift))


def over_rows(left, right):
    return lax.dot_general(
        left, right, (((0,), (0,)), ((), ())), preferred_element_type=jnp.float32
    )


def over_columns(left, right):
    return lax.dot_general(
        left, right, (((1,), (1,)), ((), ())), preferred_element_type=jnp.float32
    )


def hidden_terms(gate_sum, up_sum, back_sum):
    sigmoid = jax.nn.sigmoid(gate_sum)
    hidden = (gate_sum * sigmoid * up_sum).astype(jnp.bfloat16)
    gate_grad = (back_sum * up_sum * sigmoid * (1.0 + gate_sum * (1.0 - sigmoid))).astype(
        jnp.bfloat16
    )
    up_grad = (back_sum * gate_sum * sigmoid).astype(jnp.bfloat16)
    return (gate_grad, up_grad, hidden)


def chunk_bounds(units):
    tiles = -(-units // 128)
    edges = [min(units, 128 * (tiles * i // CHUNKS)) for i in range(CHUNKS + 1)]
    edges[-1] = units
    return list(zip(edges[:-1], edges[1:]))


def build(depth_n, row_n, col_n):
    def shards(tokens, cotangent, gate_weight, up_weight, down_weight):
        width, units = gate_weight.shape
        local = tokens.shape[0]
        count = local * row_n
        block = count // (depth_n * col_n)
        half = block * col_n
        bound = depth_n * width * TOKEN_MAX * WEIGHT_MAX
        scale = 2.0 ** math.floor(math.log2(HALF_MAX / bound))
        my_depth, my_col = lax.axis_index("depth"), lax.axis_index("col")

        col_order = doubled(col_n)
        depth_order = doubled(depth_n)
        both = jnp.stack([tokens, cotangent])
        both = jnp.concatenate(
            [both] + [from_peer(both, "row", row_n, k) for k in range(1, row_n)], axis=1
        )
        both = jnp.concatenate(
            [
                lax.dynamic_slice_in_dim(
                    both, ((my_depth ^ i) * col_n + (my_col ^ j)) * block, block, 1
                )
                for i in depth_order
                for j in col_order
            ],
            axis=1,
        )
        tok, cot = both[0], both[1]

        pieces = []
        for low, high in chunk_bounds(units):
            gate = jnp.dot(tok, gate_weight[:, low:high], preferred_element_type=jnp.float32)
            up = jnp.dot(tok, up_weight[:, low:high], preferred_element_type=jnp.float32)
            back = over_columns(cot, down_weight[low:high])
            part = jnp.stack([gate, up, back]) * scale
            total = part[:, :half]
            for k in range(1, depth_n):
                away = part[:, k * half : (k + 1) * half].astype(jnp.float16)
                total = total + swap(away, "depth", depth_n, depth_order[k]).astype(jnp.float32)
            layer = total[:, block:].astype(jnp.float16)
            total = total[:, :block]
            for k in range(1, col_n):
                away = layer[:, (k - 1) * block : k * block]
                total = total + swap(away, "col", col_n, col_order[k]).astype(jnp.float32)
            total = total * (1.0 / scale)
            whole = jnp.stack(hidden_terms(total[0], total[1], total[2]))
            for axis, n in (("col", col_n), ("depth", depth_n)):
                step = n // 2
                while step:
                    other = swap(whole, axis, n, step)
                    whole = jnp.concatenate([whole, other], axis=1)
                    step //= 2
            pieces.append(whole)
        full = jnp.concatenate(pieces, axis=2)
        gate_grad, up_grad, hidden = full[0], full[1], full[2]
        rows = over_columns(gate_grad, gate_weight) + over_columns(up_grad, up_weight)
        rows = jnp.concatenate(
            [
                lax.dynamic_slice_in_dim(
                    rows,
                    (place(my_depth ^ i, depth_n) * col_n + place(my_col ^ j, col_n)) * block,
                    block,
                    0,
                )
                for i in range(depth_n)
                for j in range(col_n)
            ],
            axis=0,
        )
        rows = rows.reshape(row_n, local, width)
        input_sum = rows[0]
        for k in range(1, row_n):
            input_sum = input_sum + lax.ppermute(
                rows[k], "row", [(i, (i + k) % row_n) for i in range(row_n)]
            )
        return (
            input_sum.astype(jnp.bfloat16),
            over_rows(tok, gate_grad).astype(jnp.bfloat16),
            over_rows(tok, up_grad).astype(jnp.bfloat16),
            over_rows(hidden, cot).astype(jnp.bfloat16),
        )

    return shards


def solution(mesh):
    return jax.shard_map(
        build(mesh.shape["depth"], mesh.shape["row"], mesh.shape["col"]),
        mesh=mesh,
        in_specs=(
            P("row", ("depth", "col")),
            P("row", ("depth", "col")),
            P(("depth", "col"), "row"),
            P(("depth", "col"), "row"),
            P("row", ("depth", "col")),
        ),
        out_specs=(
            P("row", ("depth", "col")),
            P(("depth", "col"), "row"),
            P(("depth", "col"), "row"),
            P("row", ("depth", "col")),
        ),
        check_vma=False,
    )
```
